32 devices in a mesh: dp: 4 (over x, core), space: 8 (over z, y).
Axes of the slice: x: 2, y: 2, z: 4, core: 2. Of those that a mesh axis runs over, the one named last changes fastest.
Arguments:
- section_three: bfloat16 [4, 64, 128, 512], P('dp', 'space'), parts along dimension 0, may hold values from -6 to 6
- section_four: bfloat16 [4, 32, 64, 1024], P('dp', 'space'), parts along dimension 0, may hold values from -6 to 6
- section_five: bfloat16 [4, 16, 32, 2048], P('dp', 'space'), parts along dimension 0, may hold values from -6 to 6
- lateral_three: bfloat16 [512, 256], P('space'), may hold values from -0.25 to 0.25
- lateral_four: bfloat16 [1024, 256], P('space'), may hold values from -0.1875 to 0.1875
- lateral_five: bfloat16 [2048, 256], P('space'), may hold values from -0.125 to 0.125
- lateral_bias_three: float32 [256], replicated, may hold values from -3 to 3
- lateral_bias_four: float32 [256], replicated, may hold values from -3 to 3
- lateral_bias_five: float32 [256], replicated, may hold values from -3 to 3
- output_three: bfloat16 [3, 3, 256, 256], P(None, None, 'space'), may hold values from -0.125 to 0.125
- output_four: bfloat16 [3, 3, 256, 256], P(None, None, 'space'), may hold values from -0.125 to 0.125
- output_five: bfloat16 [3, 3, 256, 256], P(None, None, 'space'), may hold values from -0.125 to 0.125
- output_bias_three: float32 [256], replicated, may hold values from -3 to 3
- output_bias_four: float32 [256], replicated, may hold values from -3 to 3
- output_bias_five: float32 [256], replicated, may hold values from -3 to 3
Outputs:
- level_three: bfloat16 [4, 64, 128, 256], P('dp', 'space'), parts along dimension 0
- level_four: bfloat16 [4, 32, 64, 256], P('dp', 'space'), parts along dimension 0
- level_five: bfloat16 [4, 16, 32, 256], P('dp'), parts along dimension 0
- level_six: bfloat16 [4, 8, 16, 256], P('dp'), parts along dimension 0
The draws below stay inside these ranges and needn't reach their ends.
There are 4 independent parts, one for each index of `dp`. The reference program is written for one: setup_inputs(seed, part) draws one part's arguments, and reference() takes and returns one part's arrays. A program takes and returns all parts, laid end to end along the dimension named above; an argument that names none is the same for every part. Nothing has to cross between parts.
All inputs are finite; a program needn't handle non-finite values.
Results may differ from the reference program's by a relative error of at most 0.0095.
Values may be sent and summed in bfloat16 or wider, within the bound.
No kernel may reach another device: no remote copies, remote signals or barrier semaphores. Data moves between devices by JAX's collectives and lax.ppermute only.
A program may use at most 64 MiB of HBM per device.

```python
import jax
import jax.numpy as jnp

C3 = 512
C4 = 1024
C5 = 2048
FD = 256
IMG = 1
W5 = 32
H5 = 16
H4 = 32
H3 = 64
W4 = 64
W3 = 128


def levels(own_key, shape, shards, low, high):
    gain, own = 1.0, jax.random.fold_in(own_key, 6)
    for dim, shards_of in shards:
        draws = jnp.exp(jax.random.uniform(jax.random.fold_in(own, dim), (shards_of,), jnp.float32, low / len(shards), high / len(shards)))
        gain = gain * jnp.repeat(draws, shape[dim] // shards_of).reshape([-1 if axis == dim else 1 for axis in range(len(shape))])
    return gain


def gaussian(key, shape, width, reach, split=(), dtype=jnp.bfloat16):
    values = width * jax.random.normal(key, shape, jnp.float32)
    if split:
        values = values * levels(key, shape, split, -0.22, 0.18)
    return jnp.clip(values, -reach, reach).astype(dtype)


def setup_inputs(seed: int = 0, part: int = 0) -> dict:
    key_of = jax.random.split(jax.random.key(seed), 16)
    part_keys = jax.random.split(jax.random.fold_in(key_of[15], part), 16)
    section_three = gaussian(part_keys[0], (IMG, H3, W3, C3), 1.0, 6.0, ((1, 8),))
    section_four = gaussian(part_keys[1], (IMG, H4, W4, C4), 1.0, 6.0, ((1, 8),))
    section_five = gaussian(part_keys[2], (IMG, H5, W5, C5), 1.0, 6.0, ((1, 8),))
    lateral_three = gaussian(key_of[3], (C3, FD), C3 ** -0.5, 0.25, ((0, 8),))
    lateral_four = gaussian(key_of[4], (C4, FD), C4 ** -0.5, 0.1875, ((0, 8),))
    lateral_five = gaussian(key_of[5], (C5, FD), C5 ** -0.5, 0.125, ((0, 8),))
    lateral_bias_three = gaussian(key_of[6], (FD,), 0.5, 3.0, (), jnp.float32)
    lateral_bias_four = gaussian(key_of[7], (FD,), 0.5, 3.0, (), jnp.float32)
    lateral_bias_five = gaussian(key_of[8], (FD,), 0.5, 3.0, (), jnp.float32)
    output_three = gaussian(key_of[9], (3, 3, FD, FD), (9 * FD) ** -0.5, 0.125, ((2, 8),))
    output_four = gaussian(key_of[10], (3, 3, FD, FD), (9 * FD) ** -0.5, 0.125, ((2, 8),))
    output_five = gaussian(key_of[11], (3, 3, FD, FD), (9 * FD) ** -0.5, 0.125, ((2, 8),))
    output_bias_three = gaussian(key_of[12], (FD,), 0.5, 3.0, (), jnp.float32)
    output_bias_four = gaussian(key_of[13], (FD,), 0.5, 3.0, (), jnp.float32)
    output_bias_five = gaussian(key_of[14], (FD,), 0.5, 3.0, (), jnp.float32)
    return dict(section_three=section_three, section_four=section_four, section_five=section_five, lateral_three=lateral_three, lateral_four=lateral_four, lateral_five=lateral_five, lateral_bias_three=lateral_bias_three, lateral_bias_four=lateral_bias_four, lateral_bias_five=lateral_bias_five, output_three=output_three, output_four=output_four, output_five=output_five, output_bias_three=output_bias_three, output_bias_four=output_bias_four, output_bias_five=output_bias_five)


def lateral(features, weight, offset):
    images, rows, columns, channels = features.shape
    summed = jnp.dot(features.reshape(-1, channels), weight, preferred_element_type=jnp.float32) + offset
    return summed.reshape(images, rows, columns, -1)


def enlarge(coarse):
    return jnp.repeat(jnp.repeat(coarse, 2, axis=1), 2, axis=2)


def conv_rows(padded, weight, offset):
    images, rows_in, columns, channels = padded.shape
    height = rows_in - 2
    framed = jnp.pad(padded, ((0, 0), (0, 0), (1, 1), (0, 0)))
    summed = jnp.zeros((images * height * columns, weight.shape[3]), jnp.float32)
    for row_off in range(3):
        for col_off in range(3):
            window = framed[:, row_off:row_off + height, col_off:col_off + columns, :].reshape(-1, channels)
            summed = summed + jnp.dot(window, weight[row_off, col_off], preferred_element_type=jnp.float32)
    return (summed + offset).reshape(images, height, columns, -1).astype(jnp.bfloat16)


def pad_rows(field):
    return jnp.pad(field, ((0, 0), (1, 1), (0, 0), (0, 0)))


def reference(section_three, section_four, section_five, lateral_three, lateral_four, lateral_five, lateral_bias_three, lateral_bias_four, lateral_bias_five, output_three, output_four, output_five, output_bias_three, output_bias_four, output_bias_five):
    merged_five = lateral(section_five, lateral_five, lateral_bias_five).astype(jnp.bfloat16)
    merged_four = (lateral(section_four, lateral_four, lateral_bias_four) + enlarge(merged_five).astype(jnp.float32)).astype(jnp.bfloat16)
    merged_three = (lateral(section_three, lateral_three, lateral_bias_three) + enlarge(merged_four).astype(jnp.float32)).astype(jnp.bfloat16)
    level_three = conv_rows(pad_rows(merged_three), output_three, output_bias_three)
    level_four = conv_rows(pad_rows(merged_four), output_four, output_bias_four)
    level_five = conv_rows(pad_rows(merged_five), output_five, output_bias_five)
    level_six = level_five[:, ::2, ::2, :]
    return (level_three, level_four, level_five, level_six)
```

```python
import functools

import jax
import jax.numpy as jnp
from jax import lax
from jax.experimental import pallas as pl
from jax.experimental.pallas import tpu as pltpu
from jax.sharding import PartitionSpec as P


LANES = 128
ANY = pl.BlockSpec(memory_space=pl.ANY)
VMEM = pl.BlockSpec(memory_space=pltpu.VMEM)


def swap(array, axis, mask):
    count = lax.axis_size(axis)
    return lax.ppermute(array, axis, [(i, i ^ mask) for i in range(count)])


def spread(piece, halves, rows_split):
    count = lax.axis_size("space")
    near = [piece] + [swap(piece, "space", 2 * k) for k in range(1, count // 2)]
    sets = [jnp.stack(near)]
    sets.append(swap(sets[0], "space", 1))
    if rows_split == 2:
        sets += [swap(held, "dp", halves) for held in sets]
    if halves == 2:
        sets += [swap(held, "dp", 1) for held in sets]
    return sets


def places(sets, halves, rows_split):
    me, other = lax.axis_index("space"), lax.axis_index("dp")
    core, side = lax.rem(other, halves), lax.rem(lax.div(other, halves), rows_split)
    found = []
    for index in range(len(sets)):
        flip_x = (index >> 1) & 1 if rows_split == 2 else 0
        flip_core = index // (2 * rows_split)
        for p in range(lax.axis_size("space") // 2):
            shard = jnp.bitwise_xor(me, 2 * p + (index & 1))
            found.append((index, p, shard, jnp.bitwise_xor(side, flip_x), jnp.bitwise_xor(core, flip_core)))
    return found


def run_all(copies):
    for copy in copies:
        copy.start()
    return copies


def wait_all(copies):
    for copy in copies:
        copy.wait()


def lateral_copies(sets, first, rows, target, halves, sem):
    width = target.shape[1] // halves
    copies = []
    for index, p, shard, _, half in places(sets, halves, 1):
        copies.append(
            pltpu.make_async_copy(
                sets[index].at[p, pl.ds(first, rows)],
                target.at[
                    pl.ds(pl.multiple_of(shard * rows, rows), rows),
                    pl.ds(pl.multiple_of(half * width, width), width),
                ],
                sem,
            )
        )
    return run_all(copies)


def output_copies(sets, level, target, halves, rows_split, sem):
    width = target.shape[3] // halves
    rows = sets[0].shape[4]
    copies = []
    for index, p, shard, part, half in places(sets, halves, rows_split):
        start = (shard * rows_split + part) * rows
        copies.append(
            pltpu.make_async_copy(
                sets[index].at[p, level],
                target.at[
                    :,
                    :,
                    pl.ds(pl.multiple_of(start, rows), rows),
                    pl.ds(pl.multiple_of(half * width, width), width),
                ],
                sem,
            )
        )
    return run_all(copies)


def doubled(rows_of, count):
    coarse = rows_of.shape[0]
    line = lax.broadcasted_iota(jnp.int32, (count, coarse), 0)
    column = lax.broadcasted_iota(jnp.int32, (count, coarse), 1)
    pick = jnp.where(lax.div(line, 2) == column, 1.0, 0.0).astype(rows_of.dtype)
    return jnp.dot(pick, rows_of, preferred_element_type=jnp.float32)


def five_kernel(halves, cells, *refs):
    section, bias = refs[:2]
    sets = refs[2 : 2 + cells]
    out, data, weight, sem, wsem = refs[2 + cells :]
    first = run_all([pltpu.make_async_copy(section, data, sem)])
    rows = weight.shape[0] // lax.axis_size("space")
    copies = lateral_copies(sets, 0, rows, weight, halves, wsem)
    wait_all(first + copies)
    total = jnp.dot(data[...], weight[...], preferred_element_type=jnp.float32)
    out[...] = (total + bias[...]).astype(out.dtype)


def merge_kernel(halves, cells, width5, first4, *refs):
    section4, section3, five, bias4, bias3 = refs[:5]
    sets = refs[5 : 5 + cells]
    out4, out3, data4, data3, weight4, weight3, sem, wsem4, wsem3 = refs[5 + cells :]
    loads = run_all(
        [
            pltpu.make_async_copy(section4, data4, sem.at[0]),
            pltpu.make_async_copy(section3, data3, sem.at[1]),
        ]
    )
    shards = lax.axis_size("space")
    rows4, rows3 = weight4.shape[0] // shards, weight3.shape[0] // shards
    copies4 = lateral_copies(sets, first4, rows4, weight4, halves, wsem4)
    copies3 = lateral_copies(sets, first4 + rows4, rows3, weight3, halves, wsem3)
    width4, width3 = 2 * width5, 4 * width5
    loads[0].wait()
    wait_all(copies4)
    for row in range(five.shape[0] // width5):
        up = doubled(five[pl.ds(row * width5, width5), :], width4)
        for twin in range(2):
            at = pl.ds((2 * row + twin) * width4, width4)
            total = jnp.dot(data4[at, :], weight4[...], preferred_element_type=jnp.float32)
            out4[at, :] = (total + bias4[...] + up).astype(out4.dtype)
    loads[1].wait()
    wait_all(copies3)
    for row in range(out4.shape[0] // width4):
        up = doubled(out4[pl.ds(row * width4, width4), :], width3)
        for twin in range(2):
            at = pl.ds((2 * row + twin) * width3, width3)
            total = jnp.dot(data3[at, :], weight3[...], preferred_element_type=jnp.float32)
            out3[at, :] = (total + bias3[...] + up).astype(out3.dtype)


def convolve(framed, weight, bias, width, start, count):
    taps, _, channels, wide = weight.shape
    cells = framed[pl.ds(start, count), :]
    parts = [
        jnp.dot(
            cells,
            weight[c].reshape(3 * channels, wide),
            preferred_element_type=jnp.float32,
        )
        for c in range(taps)
    ]
    column = lax.rem(lax.broadcasted_iota(jnp.int32, (count, wide), 0), width)
    left = jnp.where(column == 0, 0.0, pltpu.roll(parts[0], 1, 0))
    right = jnp.where(column == width - 1, 0.0, pltpu.roll(parts[2], count - 1, 0))
    return parts[1] + left + right + bias[...]


def level_five_kernel(halves, rows_split, cells, width, grids, *refs):
    bias = refs[0]
    maps = refs[1 : 1 + grids]
    sets = refs[1 + grids : 1 + grids + cells]
    out5, out6, framed, weight, full, sem, wsem = refs[1 + grids + cells :]
    channels = weight.shape[2]
    copies = output_copies(sets, 2, weight, halves, rows_split, wsem)
    me = lax.axis_index("space")
    height = out5.shape[0] // width
    moves = []
    for index, grid in enumerate(maps):
        for j in range(2):
            shard = jnp.bitwise_xor(me, 2 * index + j)
            pixels = grid.shape[1]
            for a in range(3):
                start = shard * pixels + (2 - a) * width
                moves.append(
                    pltpu.make_async_copy(
                        grid.at[j],
                        framed.at[
                            pl.ds(pl.multiple_of(start, width), pixels),
                            pl.ds(a * channels, channels),
                        ],
                        sem,
                    )
                )
    run_all(moves)
    blank = jnp.zeros((width, channels), framed.dtype)
    framed[pl.ds(width, width), pl.ds(0, channels)] = blank
    framed[pl.ds(height * width, width), pl.ds(2 * channels, channels)] = blank
    wait_all(moves + copies)
    total = convolve(framed, weight, bias, width, width, height * width)
    out5[...] = total.astype(out5.dtype)
    half = width // 2
    for column in range(full.shape[0]):
        lanes = pl.ds(column * LANES, LANES)
        full[column] = total[:, column * LANES : (column + 1) * LANES]
        for row in range(0, height, 2):
            out6[pl.ds(row // 2 * half, half), lanes] = full[
                column, pl.ds(row * width, half, stride=2), :
            ].astype(out6.dtype)


def frame_copies(grid, above, below, framed, width, channels, sem):
    pixels = grid.shape[0]
    rest = pixels - width
    pairs = [
        (grid, framed.at[:, pl.ds(channels, channels)]),
        (
            grid.at[pl.ds(0, rest)],
            framed.at[pl.ds(width, rest), pl.ds(0, channels)],
        ),
        (
            grid.at[pl.ds(width, rest)],
            framed.at[pl.ds(0, rest), pl.ds(2 * channels, channels)],
        ),
        (above, framed.at[pl.ds(0, width), pl.ds(0, channels)]),
        (below, framed.at[pl.ds(rest, width), pl.ds(2 * channels, channels)]),
    ]
    return run_all([pltpu.make_async_copy(a, b, sem) for a, b in pairs])


def levels_kernel(halves, rows_split, cells, width4, *refs):
    map4, above4, below4, map3, above3, below3, bias4, bias3 = refs[:8]
    sets = refs[8 : 8 + cells]
    out4, out3, framed4, framed3, weight4, weight3, sem, wsem = refs[8 + cells :]
    width3 = 2 * width4
    channels = weight4.shape[2]
    copies4 = output_copies(sets, 1, weight4, halves, rows_split, wsem.at[0])
    moves4 = frame_copies(map4, above4, below4, framed4, width4, channels, sem.at[0])
    copies3 = output_copies(sets, 0, weight3, halves, rows_split, wsem.at[1])
    moves3 = frame_copies(map3, above3, below3, framed3, width3, channels, sem.at[1])
    wait_all(copies4 + moves4)
    out4[...] = convolve(framed4, weight4, bias4, width4, 0, out4.shape[0]).astype(out4.dtype)
    wait_all(copies3 + moves3)
    block = out3.shape[0] // 2 if (out3.shape[0] // width3) % 2 == 0 else out3.shape[0]
    for start in range(0, out3.shape[0], block):
        out3[pl.ds(start, block), :] = convolve(
            framed3, weight3, bias3, width3, start, block
        ).astype(out3.dtype)


def call(kernel, name, operands, specs, outs, scratch, flops):
    return pl.pallas_call(
        kernel,
        name=name,
        out_shape=tuple(jax.ShapeDtypeStruct(shape, jnp.bfloat16) for shape in outs),
        in_specs=specs,
        out_specs=tuple(VMEM for _ in outs),
        scratch_shapes=scratch,
        cost_estimate=pl.CostEstimate(flops=flops, bytes_accessed=4 << 20, transcendentals=0),
    )(*operands)


def on_device(
    section_three,
    section_four,
    section_five,
    lateral_three,
    lateral_four,
    lateral_five,
    lateral_bias_three,
    lateral_bias_four,
    lateral_bias_five,
    output_three,
    output_four,
    output_five,
    output_bias_three,
    output_bias_four,
    output_bias_five,
):
    bf16 = jnp.bfloat16
    shards, groups = lax.axis_size("space"), lax.axis_size("dp")
    wide = lateral_three.shape[1]
    thin = output_three.shape[2]
    halves = 2 if groups % 2 == 0 and wide % (2 * LANES) == 0 else 1
    rows_split = 2 if groups % 4 == 0 and halves == 2 and thin % 32 == 0 else 1
    other = lax.axis_index("dp")
    core, side = lax.rem(other, halves), lax.rem(lax.div(other, halves), rows_split)
    part_cols, part_rows = wide // halves, thin // rows_split

    laterals = jnp.concatenate([lateral_five, lateral_four, lateral_three])
    lateral_piece = lax.dynamic_slice_in_dim(laterals, core * part_cols, part_cols, 1)
    outputs = jnp.stack([output_three, output_four, output_five]).transpose(0, 2, 1, 3, 4)
    output_piece = lax.dynamic_slice(
        outputs,
        (0, 0, 0, side * part_rows, core * part_cols),
        (3, 3, 3, part_rows, part_cols),
    )
    lateral_sets = spread(lateral_piece, halves, 1)
    output_sets = spread(output_piece, halves, rows_split)

    images, rows5, width5, deep5 = section_five.shape
    rows4, width4, deep4 = section_four.shape[1:]
    rows3, width3, deep3 = section_three.shape[1:]
    pixels5, pixels4, pixels3 = rows5 * width5, rows4 * width4, rows3 * width3
    row = lambda bias: bias.reshape(1, -1)
    dma = pltpu.SemaphoreType.DMA

    (merged_five,) = call(
        functools.partial(five_kernel, halves, len(lateral_sets)),
        "merge_five",
        (section_five.reshape(pixels5, deep5), row(lateral_bias_five), *lateral_sets),
        [ANY, VMEM] + [ANY] * len(lateral_sets),
        [(pixels5, wide)],
        [
            pltpu.VMEM((pixels5, deep5), bf16),
            pltpu.VMEM((deep5, wide), bf16),
            dma,
            dma,
        ],
        2 * pixels5 * deep5 * wide,
    )
    pair = jnp.stack([merged_five, swap(merged_five, "space", 1)])
    grids = [pair] + [swap(pair, "space", 2 * k) for k in range(1, shards // 2)]

    merged_four, merged_three = call(
        functools.partial(
            merge_kernel, halves, len(lateral_sets), width5, lateral_five.shape[0]
        ),
        "merge_rest",
        (
            section_four.reshape(pixels4, deep4),
            section_three.reshape(pixels3, deep3),
            merged_five,
            row(lateral_bias_four),
            row(lateral_bias_three),
            *lateral_sets,
        ),
        [ANY, ANY, VMEM, VMEM, VMEM] + [ANY] * len(lateral_sets),
        [(pixels4, wide), (pixels3, wide)],
        [
            pltpu.VMEM((pixels4, deep4), bf16),
            pltpu.VMEM((pixels3, deep3), bf16),
            pltpu.VMEM((deep4, wide), bf16),
            pltpu.VMEM((deep3, wide), bf16),
            dma((2,)),
            dma,
            dma,
        ],
        2 * (pixels4 * deep4 + pixels3 * deep3) * wide,
    )

    down = [(i, i + 1) for i in range(shards - 1)]
    up = [(i + 1, i) for i in range(shards - 1)]
    above4 = lax.ppermute(merged_four[pixels4 - width4 :], "space", down)
    below4 = lax.ppermute(merged_four[:width4], "space", up)
    above3 = lax.ppermute(merged_three[pixels3 - width3 :], "space", down)
    below3 = lax.ppermute(merged_three[:width3], "space", up)

    total5 = shards * pixels5
    level_five, level_six = call(
        functools.partial(
            level_five_kernel, halves, rows_split, len(output_sets), width5, len(grids)
        ),
        "level_five",
        (row(output_bias_five), *grids, *output_sets),
        [VMEM] + [ANY] * (len(grids) + len(output_sets)),
        [(total5, wide), (total5 // 4, wide)],
        [
            pltpu.VMEM((total5 + 2 * width5, 3 * wide), bf16),
            pltpu.VMEM((3, 3, wide, wide), bf16),
            pltpu.VMEM((wide // LANES, total5, LANES), jnp.float32),
            dma,
            dma,
        ],
        18 * total5 * wide * wide,
    )
    level_four, level_three = call(
        functools.partial(levels_kernel, halves, rows_split, len(output_sets), width4),
        "levels_rest",
        (
            merged_four,
            above4,
            below4,
            merged_three,
            above3,
            below3,
            row(output_bias_four),
            row(output_bias_three),
            *output_sets,
        ),
        [ANY] * 6 + [VMEM] * 2 + [ANY] * len(output_sets),
        [(pixels4, wide), (pixels3, wide)],
        [
            pltpu.VMEM((pixels4, 3 * wide), bf16),
            pltpu.VMEM((pixels3, 3 * wide), bf16),
            pltpu.VMEM((3, 3, wide, wide), bf16),
            pltpu.VMEM((3, 3, wide, wide), bf16),
            dma((2,)),
            dma((2,)),
        ],
        18 * (pixels4 + pixels3) * wide * wide,
    )
    high = shards * rows5
    return (
        level_three.reshape(images, rows3, width3, wide),
        level_four.reshape(images, rows4, width4, wide),
        level_five.reshape(images, high, width5, wide),
        level_six.reshape(images, high // 2, width5 // 2, wide),
    )


def solution(mesh):
    return jax.shard_map(
        on_device,
        mesh=mesh,
        in_specs=(
            P("dp", "space", None, None),
            P("dp", "space", None, None),
            P("dp", "space", None, None),
            P("space", None),
            P("space", None),
            P("space", None),
            P(),
            P(),
            P(),
            P(None, None, "space", None),
            P(None, None, "space", None),
            P(None, None, "space", None),
            P(),
            P(),
            P(),
        ),
        out_specs=(
            P("dp", "space", None, None),
            P("dp", "space", None, None),
            P("dp", None, None, None),
            P("dp", None, None, None),
        ),
        check_vma=False,
    )
```
